32 devices in a mesh: mb: 4 (over z), tp: 2 (over y), dp: 4 (over x, core).
Axes of the slice: x: 2, y: 2, z: 4, core: 2. Of those that a mesh axis runs over, the one named last changes fastest.
Arguments:
- hidden: bfloat16 [4, 8, 512, 7168], P('dp', 'mb', None, 'tp'), may hold values from -6 to 6
- latent: bfloat16 [4, 8, 512, 512], P('dp', 'mb', None, 'tp'), may hold values from -6 to 6
- out_grad: bfloat16 [4, 8, 512, 16384], P('dp', 'mb', None, 'tp'), may hold values from -0.059814453 to 0.059814453
- up_weight: bfloat16 [512, 16384], P(None, 'tp'), may hold values from -0.046875 to 0.046875
- mb_tokens: int32 [4, 8], P('dp'), may hold values from 128 to 512, as said below
- slot_mb: int32 [4, 8], P('dp', 'mb'), may hold values from 0 to 7, each once within a row
Outputs:
- up_grad: float32 [512, 16384], P(('mb', 'dp'), 'tp')
- running_down: float32 [4, 7168, 512], P('mb', 'tp', 'dp')
The draws below stay inside these ranges and needn't reach their ends.
Inputs may be any that keep to these rules, and one draw needn't show every extreme that they name: `mb_tokens`: each count is a multiple of 128; in every group some microbatch has exactly 512 tokens. `slot_mb`: each row is a permutation of the microbatch numbers.
All inputs are finite; a program needn't handle non-finite values.
Results may differ from the reference program's by a relative error of at most 0.005.
Values may be sent and summed in bfloat16 or wider, within the bound.
No kernel may reach another device: no remote copies, remote signals or barrier semaphores. Data moves between devices by JAX's collectives and lax.ppermute only.
A program may use at most 128 MiB of HBM per device.

```python
import jax
import jax.numpy as jnp
from jax import lax

D = 7168
R = 512
COLS = 16384
TOKBLOCK = 128
CAP = 512
SLOTS = 2
MICRO = 8
GROUPS = 4
N_MB = 4


def draw_mb_tokens(key, part):
    first_key, second_key = jax.random.split(jax.random.fold_in(key, 11))
    blocks = jax.random.randint(first_key, (GROUPS, MICRO), 1, CAP // TOKBLOCK + 1)
    chosen = jax.random.randint(second_key, (GROUPS, 1), 0, MICRO)
    blocks = jnp.where(jnp.arange(MICRO)[None, :] == chosen, CAP // TOKBLOCK, blocks)
    return (blocks * TOKBLOCK).astype(jnp.int32)


def block_scale(own_key, dims, cuts, smallest, top_value):
    level, own = 1.0, jax.random.fold_in(own_key, 6)
    for axis_at, shards_of in cuts:
        steps = jnp.exp(jax.random.uniform(jax.random.fold_in(own, axis_at), (shards_of,), jnp.float32, smallest / len(cuts), top_value / len(cuts)))
        level = level * jnp.repeat(steps, dims[axis_at] // shards_of).reshape([-1 if axis == axis_at else 1 for axis in range(len(dims))])
    return level


def noise(rng, shape, scale, limit, cuts=(), kind=jnp.bfloat16):
    values = jax.random.normal(rng, shape, jnp.float32) * scale
    if len(cuts) > 0:
        values = block_scale(rng, shape, cuts, -0.22, 0.18) * values
    return jnp.clip(values, min=-limit, max=limit).astype(kind)


def setup_inputs(seed: int = 0) -> dict:
    key_of = jax.random.split(jax.random.key(seed), 7)
    return {
        "hidden": noise(key_of[0], (GROUPS, MICRO, CAP, D), 1.0, 6.0, ((0, 4), (1, 4), (3, 2))),
        "latent": noise(key_of[1], (GROUPS, MICRO, CAP, R), 1.0, 6.0, ((0, 4), (1, 4), (3, 2))),
        "out_grad": noise(key_of[2], (GROUPS, MICRO, CAP, COLS), 0.01, 0.059814453, ((0, 4), (1, 4), (3, 2))),
        "up_weight": noise(key_of[3], (R, COLS), COLS ** -0.5, 0.046875, ((1, 2),)),
        "mb_tokens": draw_mb_tokens(jax.random.fold_in(key_of[6], 71), 0),
        "slot_mb": jax.vmap(lambda own: jax.random.permutation(own, MICRO))(jax.random.split(key_of[5], GROUPS)).reshape((GROUPS, MICRO)).astype(jnp.int32),
    }


def reference(hidden, latent, out_grad, up_weight, mb_tokens, slot_mb):
    counts = jnp.take_along_axis(mb_tokens, slot_mb, axis=1).reshape(-1)
    owners = jnp.tile(jnp.arange(MICRO, dtype=jnp.int32) // SLOTS, GROUPS)
    positions = jnp.arange(CAP, dtype=jnp.int32)

    def accumulate(carry, inputs_now):
        up_total, down_owner = carry
        hidden_rows, latent_rows, grad_rows, length, owner_id = inputs_now
        masked = jnp.where((positions < length)[:, None], grad_rows, jnp.zeros((), grad_rows.dtype))
        latent_grad = jnp.dot(masked, up_weight.T, preferred_element_type=jnp.float32).astype(jnp.bfloat16)
        up_total = up_total + jnp.dot(latent_rows.T, masked, preferred_element_type=jnp.float32)
        down_term = jnp.dot(hidden_rows.T, latent_grad, preferred_element_type=jnp.float32)
        down_owner = down_owner.at[owner_id].add(down_term)
        return (up_total, down_owner), None

    start_state = (jnp.zeros((R, COLS), jnp.float32), jnp.zeros((N_MB, D, R), jnp.float32))
    sequence = (hidden.reshape(-1, CAP, D), latent.reshape(-1, CAP, R), out_grad.reshape(-1, CAP, COLS), counts, owners)
    (up_total, down_owner), unused = lax.scan(accumulate, start_state, sequence)
    return up_total, jnp.cumsum(down_owner, axis=0)
```

```python
import functools

import jax
import jax.numpy as jnp
from jax import lax
from jax.sharding import PartitionSpec as P


UP_CHUNKS = 2
DOWN_CHUNKS = 2


def swap(value, axis, size, flip):
    return lax.ppermute(value, axis, [(i, i ^ flip) for i in range(size)])


def shift(value, axis, size, step):
    return lax.ppermute(value, axis, [(i, (i + step) % size) for i in range(size)])


def halve(pieces, axis, size):
    bit = 1
    while bit < size:
        keys = sorted(pieces)
        sent = [k for k in keys if k & bit]
        kept = [k for k in keys if not k & bit]
        arrived = swap(jnp.concatenate([pieces[k].astype(jnp.bfloat16) for k in sent], 0), axis, size, bit)
        rows = arrived.shape[0] // len(sent)
        pieces = {
            k: pieces[k].astype(jnp.float32) + arrived[n * rows:(n + 1) * rows].astype(jnp.float32)
            for n, k in enumerate(kept)
        }
        bit *= 2
    return pieces[0]


def local(n_mb, n_tp, n_dp, hidden, latent, out_grad, up_weight, mb_tokens, slot_mb):
    slots, cap = hidden.shape[1], hidden.shape[2]
    rows = slots * cap
    micro = mb_tokens.shape[1]
    rank = up_weight.shape[0]
    cols = up_weight.shape[1]
    local_rank = latent.shape[3]
    width = hidden.shape[3]
    block = rank // (n_mb * n_dp)
    my_mb = lax.axis_index("mb")
    my_tp = lax.axis_index("tp")
    my_dp = lax.axis_index("dp")
    f32, bf16 = jnp.float32, jnp.bfloat16

    lookup = slot_mb[0][:, None] == jnp.arange(micro, dtype=jnp.int32)[None, :]
    counts = jnp.sum(jnp.where(lookup, mb_tokens[0][None, :], 0), axis=1)
    live = jnp.arange(cap, dtype=jnp.int32)[None, :] < counts[:, None]
    grads = out_grad[0].reshape(rows, cols)

    own = jnp.where(live[:, :, None], latent[0], jnp.zeros((), bf16)).reshape(rows, local_rank)
    shares = [own] + [swap(own, "tp", n_tp, t) for t in range(1, n_tp)]

    lat = []
    for s in range(slots):
        part = lax.dot_general(out_grad[0, s], up_weight, (((1,), (1,)), ((), ())), preferred_element_type=f32)
        bit = 1
        while bit < n_tp:
            part = part + swap(part.astype(bf16), "tp", n_tp, bit).astype(f32)
            bit *= 2
        lat.append(jnp.where(live[s][:, None], part, 0.0).astype(bf16))
    latent_grad = jnp.concatenate(lat, 0)

    order = [k for k in range(n_dp) if k & 1] + [k for k in range(n_dp) if not k & 1]
    kk = jnp.asarray(order, jnp.int32)[:, None, None]
    jj = jnp.arange(n_mb, dtype=jnp.int32)[None, :, None]
    bb = jnp.arange(block, dtype=jnp.int32)[None, None, :]
    source = ((((my_mb + jj) % n_mb) * n_dp + (my_dp ^ kk)) * block + bb).reshape(rank)
    factors = jnp.zeros((rank, rows), f32)
    for t, share in enumerate(shares):
        pick = source[:, None] == (my_tp ^ t) * local_rank + jnp.arange(local_rank, dtype=jnp.int32)[None, :]
        factors = factors + lax.dot_general(
            pick.astype(bf16), share, (((1,), (1,)), ((), ())), preferred_element_type=f32
        )
    factors = factors.astype(bf16)
    odd = len([k for k in order if k & 1])
    per = n_mb * block

    def up_chunk(c):
        size = cols // UP_CHUNKS
        g = grads[:, c * size:(c + 1) * size]
        out = {}
        for group, first in ((order[:odd], 0), (order[odd:], odd)):
            if not group:
                continue
            u = jnp.dot(
                factors[first * per:(first + len(group)) * per], g,
                preferred_element_type=bf16 if first == 0 and odd else f32,
            )
            for n, k in enumerate(group):
                out[k] = u[n * per:(n + 1) * per]
        total = halve(out, "dp", n_dp)
        acc = total[:block]
        for j in range(1, n_mb):
            acc = acc + shift(total[j * block:(j + 1) * block].astype(bf16), "mb", n_mb, j).astype(f32)
        return acc

    def down_chunk(c):
        size = width // DOWN_CHUNKS
        h = hidden[0, :, :, c * size:(c + 1) * size].reshape(rows, size)
        share = rank // n_dp
        out = {}
        for group in ([k for k in range(n_dp) if k & 1], [k for k in range(n_dp) if not k & 1]):
            if not group:
                continue
            want = jnp.concatenate(
                [lax.dynamic_slice_in_dim(latent_grad, (my_dp ^ k) * share, share, 1) for k in group], 1)
            d = lax.dot_general(h, want, (((0,), (0,)), ((), ())), preferred_element_type=f32)
            for n, k in enumerate(group):
                out[k] = d[:, n * share:(n + 1) * share]
        term = halve(out, "dp", n_dp)
        carry = jnp.zeros_like(term)
        for s in range(n_mb - 1):
            moved = lax.ppermute((term + carry).astype(bf16), "mb", [(s, s + 1)])
            carry = carry + moved.astype(f32)
        return term + carry

    ups = [up_chunk(0)]
    downs = [down_chunk(c) for c in range(DOWN_CHUNKS)]
    ups += [up_chunk(c) for c in range(1, UP_CHUNKS)]
    return (jnp.concatenate(ups, 1), jnp.concatenate(downs, 0)[None])


def solution(mesh):
    sizes = mesh.shape
    return jax.shard_map(
        functools.partial(local, sizes["mb"], sizes["tp"], sizes["dp"]),
        mesh=mesh,
        in_specs=(
            P("dp", "mb", None, "tp"),
            P("dp", "mb", None, "tp"),
            P("dp", "mb", None, "tp"),
            P(None, "tp"),
            P("dp", None),
            P("dp", "mb"),
        ),
        out_specs=(P(("mb", "dp"), "tp"), P("mb", "tp", "dp")),
        check_vma=False,
    )
```
